32 devices in a mesh: data: 2 (over x), dap2: 4 (over z), dap: 4 (over y, core).
Axes of the slice: x: 2, y: 2, z: 4, core: 2. Of those that a mesh axis runs over, the one named last changes fastest.
Arguments:
- pair_act: float32 [1280, 640, 128], P(('data', 'dap'), 'dap2'), parts along dimension 0
- pair_mask: int32 [1280, 640], P(('data', 'dap'), 'dap2'), parts along dimension 0
- ln_z: bfloat16 [1, 2, 2, 128], replicated
- w_ab: bfloat16 [1, 2, 128, 512], replicated
- w_g: bfloat16 [1, 2, 128, 128], replicated
- ln_x: bfloat16 [1, 2, 2, 128], replicated
- w_o: bfloat16 [1, 2, 128, 128], replicated
Outputs:
- output: float32 [1280, 640, 128], P(('data', 'dap'), 'dap2'), parts along dimension 0
There are 2 independent parts. The reference program is written for one: setup_inputs(seed, part) draws one part's arguments, and reference() takes and returns one part's arrays. A program takes and returns all parts, laid end to end along the dimension named above; an argument that names none is the same for every part.
All inputs are finite; a program needn't handle non-finite values.
Results may differ from the reference program's by a relative error of at most 0.00132326.
Values are sent between devices in bfloat16 or wider.
A program may use at most 1 GiB of HBM per device.

```python
import jax
import jax.numpy as jnp
from jax import lax

N_RES = 640
C_Z = 128
C_HID = 128
LAYERS = 1
ROW_BLOCK = 64
LN_EPS = 1e-5


def norm_params(base_key, width):
    key_gain, key_bias = jax.random.split(base_key)
    gain = 1.0 + 0.3 * jax.random.normal(key_gain, (LAYERS, 2, 1, width), jnp.float32)
    bias = 0.3 * jax.random.normal(key_bias, (LAYERS, 2, 1, width), jnp.float32)
    return jnp.concatenate([gain, bias], axis=2).astype(jnp.bfloat16)


def setup_inputs(seed: int = 0, part: int = 0) -> dict:
    part_key = jax.random.fold_in(jax.random.key(seed), part)
    key_act, key_len, key_hole = jax.random.split(part_key, 3)
    key_lnz, key_ab, key_gate, key_lnx, key_out = jax.random.split(jax.random.key(seed + 1), 5)
    pair_act = jax.random.normal(key_act, (N_RES, N_RES, C_Z), jnp.float32)
    valid_len = jax.random.randint(key_len, (), N_RES - N_RES // 8, N_RES - N_RES // 16 + 1)
    hole_draw = jax.random.randint(key_hole, (N_RES, N_RES), 0, 32)
    inside = jnp.arange(N_RES) < valid_len
    pair_mask = (inside[:, None] & inside[None, :] & (hole_draw != 0)).astype(jnp.int32)
    w_ab = (jax.random.normal(key_ab, (LAYERS, 2, C_Z, 4 * C_HID), jnp.float32) * C_Z ** -0.5).astype(jnp.bfloat16)
    w_g = (jax.random.normal(key_gate, (LAYERS, 2, C_Z, C_Z), jnp.float32) * C_Z ** -0.5).astype(jnp.bfloat16)
    w_o = (jax.random.normal(key_out, (LAYERS, 2, C_HID, C_Z), jnp.float32) * (C_HID * LAYERS) ** -0.5).astype(jnp.bfloat16)
    return {"pair_act": pair_act, "pair_mask": pair_mask, "ln_z": norm_params(key_lnz, C_Z), "w_ab": w_ab, "w_g": w_g, "ln_x": norm_params(key_lnx, C_HID), "w_o": w_o}


def layer_norm(values, params):
    mean = jnp.mean(values, axis=-1, keepdims=True)
    centered = values - mean
    variance = jnp.mean(centered * centered, axis=-1, keepdims=True)
    scaled = centered * lax.rsqrt(variance + LN_EPS)
    return (scaled * params[0].astype(jnp.float32) + params[1].astype(jnp.float32)).astype(jnp.bfloat16)


def project_rows(z_rows, mask_rows, ln_params, w_ab):
    z_norm = layer_norm(z_rows, ln_params)
    projected = jnp.dot(z_norm.reshape(-1, C_Z), w_ab, preferred_element_type=jnp.float32).reshape(ROW_BLOCK, N_RES, 4 * C_HID)
    keep_mask = mask_rows.astype(jnp.float32)[:, :, None]
    a_proj = (keep_mask * jax.nn.sigmoid(projected[:, :, C_HID:2 * C_HID]) * projected[:, :, :C_HID]).astype(jnp.bfloat16)
    b_proj = (keep_mask * jax.nn.sigmoid(projected[:, :, 3 * C_HID:]) * projected[:, :, 2 * C_HID:3 * C_HID]).astype(jnp.bfloat16)
    return a_proj, b_proj


def tri_update(pair_state, pair_mask, ln_z, w_ab, w_g, ln_x, w_o, outgoing):
    n_blocks = N_RES // ROW_BLOCK
    z_blocks = pair_state.reshape(n_blocks, ROW_BLOCK, N_RES, C_Z)
    mask_blocks = pair_mask.reshape(n_blocks, ROW_BLOCK, N_RES)

    def project_block(block_pair):
        return project_rows(block_pair[0], block_pair[1], ln_z, w_ab)

    a_all, b_all = lax.map(project_block, (z_blocks, mask_blocks))
    a_all = a_all.reshape(N_RES, N_RES, C_HID)
    b_all = b_all.reshape(N_RES, N_RES, C_HID)
    if not outgoing:
        a_all = jnp.swapaxes(a_all, 0, 1)
        b_all = jnp.swapaxes(b_all, 0, 1)
    b_wide = b_all.astype(jnp.float32)

    def finish_block(block_pair):
        z_rows, a_rows = block_pair
        x_sum = jnp.einsum("ikc,jkc->ijc", a_rows.astype(jnp.float32), b_wide)
        x_norm = layer_norm(x_sum, ln_x)
        update_val = jnp.dot(x_norm.reshape(-1, C_HID), w_o, preferred_element_type=jnp.float32).reshape(ROW_BLOCK, N_RES, C_Z)
        z_norm = layer_norm(z_rows, ln_z)
        gate_val = jax.nn.sigmoid(jnp.dot(z_norm.reshape(-1, C_Z), w_g, preferred_element_type=jnp.float32)).reshape(ROW_BLOCK, N_RES, C_Z)
        return z_rows + gate_val * update_val

    new_blocks = lax.map(finish_block, (z_blocks, a_all.reshape(n_blocks, ROW_BLOCK, N_RES, C_HID)))
    return new_blocks.reshape(N_RES, N_RES, C_Z)


def reference(pair_act, pair_mask, ln_z, w_ab, w_g, ln_x, w_o):
    def one_layer(pair_state, layer_params):
        ln_z_layer, w_ab_layer, w_g_layer, ln_x_layer, w_o_layer = layer_params
        pair_state = tri_update(pair_state, pair_mask, ln_z_layer[0], w_ab_layer[0], w_g_layer[0], ln_x_layer[0], w_o_layer[0], True)
        pair_state = tri_update(pair_state, pair_mask, ln_z_layer[1], w_ab_layer[1], w_g_layer[1], ln_x_layer[1], w_o_layer[1], False)
        return pair_state, None

    pair_out, _ = lax.scan(one_layer, pair_act, (ln_z, w_ab, w_g, ln_x, w_o))
    return pair_out
```

```python
import functools

import jax
import jax.numpy as jnp
from jax import lax
from jax.experimental import pallas as pl
from jax.experimental.pallas import tpu as pltpu
from jax.sharding import PartitionSpec as P

LN_EPS = 1e-5
GROUP = 16
CHAN_BLOCK = 16
CHUNKS = 8
F32 = jnp.float32
BF16 = jnp.bfloat16
MESH = pl.DeviceIdType.MESH


def sigmoid(v):
    return 0.5 * jnp.tanh(0.5 * v) + 0.5


def layer_norm_rows(v, params):
    mean = jnp.mean(v, axis=-1, keepdims=True)
    centered = v - mean
    variance = jnp.mean(centered * centered, axis=-1, keepdims=True)
    return centered * lax.rsqrt(variance + LN_EPS) * params[0:1, :] + params[1:2, :]


def norm_kernel(slot_ref, z_ref, mask_ref, ln_ref, out_ref):
    ln = ln_ref[...]
    mask = mask_ref[0]
    for ii in range(GROUP):
        zn = layer_norm_rows(z_ref[ii], ln) * mask[:, ii:ii + 1]
        out_ref[0, ii] = zn.astype(BF16)


def first_norm(z, mask_g, ln, slot, n_slots):
    rows, cols, width = z.shape
    return pl.pallas_call(
        norm_kernel,
        out_shape=jax.ShapeDtypeStruct((n_slots, rows, cols, width), BF16),
        grid_spec=pltpu.PrefetchScalarGridSpec(
            num_scalar_prefetch=1,
            grid=(rows // GROUP,),
            in_specs=[
                pl.BlockSpec((GROUP, cols, width), lambda g, s: (g, 0, 0)),
                pl.BlockSpec((1, cols, GROUP), lambda g, s: (g, 0, 0)),
                pl.BlockSpec((2, width), lambda g, s: (0, 0)),
            ],
            out_specs=pl.BlockSpec((1, GROUP, cols, width), lambda g, s: (s[0], g, 0, 0)),
        ),
        name="first_norm",
    )(slot, z, mask_g, ln)


def chunk_of(ref, slot, h, step):
    return ref.at[slot, pl.ds(h * step, step)]


def greet(z, r, n_z):
    barrier = pltpu.get_barrier_semaphore()

    def hello(where):
        pl.semaphore_signal(barrier, inc=1, device_id=where, device_id_type=MESH)

    for m in (1, 2, 3):
        hello({"dap": r ^ m})
    pl.when(z > 0)(lambda: hello({"dap2": z - 1}))
    pl.when(z < n_z - 1)(lambda: hello({"dap2": z + 1}))
    inner = (z > 0) & (z < n_z - 1)
    pl.when(inner)(lambda: pl.semaphore_wait(barrier, 5))
    pl.when(jnp.logical_not(inner))(lambda: pl.semaphore_wait(barrier, 4))


def copy_to(buf, src, dst, h, step, send_sem, recv_sem, where):
    return pltpu.make_async_remote_copy(
        src_ref=chunk_of(buf, src, h, step),
        dst_ref=chunk_of(buf, dst, h, step),
        send_sem=send_sem,
        recv_sem=recv_sem,
        device_id=where,
        device_id_type=MESH,
    )


def line_copies(buf, z, step, n_z, send_r, send_l, recv_z):
    def right(slot, h):
        return copy_to(buf, slot, slot, h, step, send_r.at[slot, h], recv_z.at[slot, h], {"dap2": z + 1})

    def left(slot, h):
        return copy_to(buf, slot, slot, h, step, send_l.at[slot, h], recv_z.at[slot, h], {"dap2": z - 1})

    return right, left


def start_line(right, left, z, n_z):
    @pl.loop(0, CHUNKS)
    def _(h):
        pl.when(z < n_z - 1)(lambda: right(z, h).start())
        pl.when(z > 0)(lambda: left(z, h).start())


def arrive_line(right, left, z, t, h, n_z, on_arrival):
    @pl.when(z - t >= 0)
    def _():
        right(z - t, h).wait_recv()
        pl.when(z < n_z - 1)(lambda: right(z - t, h).start())
        on_arrival(z - t, h)

    @pl.when(z + t < n_z)
    def _():
        left(z + t, h).wait_recv()
        pl.when(z > 0)(lambda: left(z + t, h).start())
        on_arrival(z + t, h)


def drain_line(right, left, z, n_z):
    for t in range(n_z):
        @pl.loop(0, CHUNKS)
        def _(h):
            pl.when((z - t >= 0) & (z < n_z - 1))(lambda: right(z - t, h).wait_send())
            pl.when((z + t < n_z) & (z > 0))(lambda: left(z + t, h).wait_send())


def relay_out_kernel(n_z, src_ref, buf, send_r, send_l, recv_z, send_p, send_q, recv_b, send_f):
    z = lax.axis_index("dap2")
    r = lax.axis_index("dap")
    step = buf.shape[1] // CHUNKS
    greet(z, r, n_z)
    right, left = line_copies(buf, z, step, n_z, send_r, send_l, recv_z)

    def to_near(slot, h):
        return copy_to(buf, slot, n_z + slot, h, step, send_p.at[slot, h], recv_b.at[slot, h], {"dap": r ^ 1})

    def to_far(slot, h):
        return copy_to(buf, slot, n_z + slot, h, step, send_q.at[slot, h], recv_b.at[slot, h], {"dap": r ^ 2})

    def onward(slot, h):
        return copy_to(buf, n_z + slot, n_z + slot, h, step, send_f.at[slot, h], recv_b.at[slot, h], {"dap": r ^ 1})

    def spread(slot, h):
        @pl.when(r == z)
        def _():
            to_far(slot, h).start()
            to_near(slot, h).start()

    def pass_on(slot, h):
        @pl.when(r == z ^ 2)
        def _():
            onward(slot, h).wait_recv()
            onward(slot, h).start()

    def pass_on_step(t, h):
        pl.when(z - t >= 0)(lambda: pass_on(z - t, h))
        pl.when(z + t < n_z)(lambda: pass_on(z + t, h))

    start_line(right, left, z, n_z)
    pl.loop(0, CHUNKS)(lambda h: spread(z, h))
    for t in range(1, n_z):
        @pl.loop(0, CHUNKS)
        def _(h):
            arrive_line(right, left, z, t, h, n_z, spread)
            if t == 1:
                pass_on(z, h)

                @pl.when(h >= 2)
                def _():
                    pass_on_step(1, h - 2)
            else:
                @pl.when(h >= 2)
                def _():
                    pass_on_step(t, h - 2)

                @pl.when(h < 2)
                def _():
                    pass_on_step(t - 1, h + CHUNKS - 2)
    for h in (CHUNKS - 2, CHUNKS - 1):
        pass_on_step(n_z - 1, h)
    drain_line(right, left, z, n_z)
    for slot in range(n_z):
        @pl.loop(0, CHUNKS)
        def _(h):
            @pl.when(r == z)
            def _():
                to_far(slot, h).wait_send()
                to_near(slot, h).wait_send()

            @pl.when(r == z ^ 2)
            def _():
                onward(slot, h).wait_send()

            @pl.when((r == z ^ 1) | (r == z ^ 3))
            def _():
                onward(slot, h).wait_recv()


def relay_in_kernel(n_z, src_ref, buf, send_r, send_l, recv_z, send_a, recv_a, send_p, send_q, recv_b, send_f):
    z = lax.axis_index("dap2")
    r = lax.axis_index("dap")
    step = buf.shape[1] // CHUNKS
    greet(z, r, n_z)
    right, left = line_copies(buf, z, step, n_z, send_r, send_l, recv_z)

    def to_owner(slot, h):
        return copy_to(buf, slot, n_z + r, h, step, send_a.at[slot, h], recv_a.at[r, h], {"dap": slot})

    def from_peer(peer, h):
        return copy_to(buf, r, n_z + peer, h, step, send_a.at[peer, h], recv_a.at[peer, h], {"dap": peer})

    def to_near(h):
        return copy_to(buf, z, 2 * n_z + r, h, step, send_p.at[h], recv_b.at[r, h], {"dap": r ^ 1})

    def to_far(h):
        return copy_to(buf, z, 2 * n_z + r, h, step, send_q.at[h], recv_b.at[r, h], {"dap": r ^ 2})

    def onward(h):
        return copy_to(buf, 2 * n_z + (r ^ 2), 2 * n_z + (r ^ 2), h, step, send_f.at[h], recv_b.at[r ^ 2, h], {"dap": r ^ 1})

    def from_b(peer, h):
        return copy_to(buf, z, 2 * n_z + peer, h, step, send_p.at[h], recv_b.at[peer, h], {"dap": r ^ 1})

    def spread(slot, h):
        @pl.when(slot != r)
        def _():
            to_owner(slot, h).start()

    start_line(right, left, z, n_z)

    @pl.loop(0, CHUNKS)
    def _(h):
        to_far(h).start()
        to_near(h).start()

    for t in range(1, n_z):
        @pl.loop(0, CHUNKS)
        def _(h):
            arrive_line(right, left, z, t, h, n_z, spread)
            if t == 2:
                onward(h).wait_recv()
                onward(h).start()

    drain_line(right, left, z, n_z)

    @pl.loop(0, CHUNKS)
    def _(h):
        to_far(h).wait_send()
        to_near(h).wait_send()
        onward(h).wait_send()
        from_b(r ^ 1, h).wait_recv()
        from_b(r ^ 3, h).wait_recv()
        for slot in range(n_z):
            @pl.when((slot != z) & (slot != r))
            def _():
                to_owner(slot, h).wait_send()
        for m in (1, 2, 3):
            @pl.when(r != z)
            def _():
                from_peer(r ^ m, h).wait_recv()


def relay(kernel, buf, sems, collective_id, name):
    return pl.pallas_call(
        kernel,
        out_shape=jax.ShapeDtypeStruct(buf.shape, buf.dtype),
        in_specs=[pl.BlockSpec(memory_space=pl.ANY)],
        out_specs=pl.BlockSpec(memory_space=pl.ANY),
        scratch_shapes=[pltpu.SemaphoreType.DMA(s) for s in sems],
        input_output_aliases={0: 0},
        compiler_params=pltpu.CompilerParams(collective_id=collective_id, has_side_effects=True),
        name=name,
    )(buf)


def project_kernel(slots_ref, x0, x1, x2, x3, w_ref, out_ref, stage):
    hidden = out_ref.shape[1]
    parts = out_ref.shape[3] // 128
    w_t = w_ref[0]

    def one_row(ii, carry):
        zn = jnp.concatenate([x[0, ii] for x in (x0, x1, x2, x3)], axis=0)
        q = lax.dot_general(w_t, zn, (((1,), (1,)), ((), ())), preferred_element_type=F32)
        val = sigmoid(q[hidden:]) * q[:hidden]
        for p in range(parts):
            stage[p, pl.ds(ii, hidden, stride=GROUP), :] = val[:, p * 128:(p + 1) * 128]
        return carry

    lax.fori_loop(0, GROUP, one_row, 0, unroll=2)
    for p in range(parts):
        out_ref[0, :, :, p * 128:(p + 1) * 128] = stage[p].reshape(hidden, GROUP, 128).astype(BF16)


def project(buf, slots, w_abt):
    _, rows, cols, width = buf.shape
    hidden = w_abt.shape[1] // 2
    depth = 4 * cols

    def block(k):
        return pl.BlockSpec((1, GROUP, cols, width), lambda o, g, s: (s[4 * o + k], g, 0, 0))

    return pl.pallas_call(
        project_kernel,
        out_shape=jax.ShapeDtypeStruct((2, hidden, rows, depth), BF16),
        grid_spec=pltpu.PrefetchScalarGridSpec(
            num_scalar_prefetch=1,
            grid=(2, rows // GROUP),
            in_specs=[block(0), block(1), block(2), block(3), pl.BlockSpec((1, 2 * hidden, width), lambda o, g, s: (o, 0, 0))],
            out_specs=pl.BlockSpec((1, hidden, GROUP, depth), lambda o, g, s: (o, 0, g, 0)),
            scratch_shapes=[pltpu.VMEM((depth // 128, hidden * GROUP, 128), F32)],
        ),
        name="project",
    )(slots, buf, buf, buf, buf, w_abt)


def finish_kernel(n_mul, emit, slot_ref, a_ref, b_ref, z_ref, lnz_ref, wg_ref, lnx_ref, wo_ref, *rest):
    if emit:
        mask_ref, ln2_ref, out_ref, next_ref, x_lo, x_hi, turn = rest
    else:
        out_ref, x_lo, x_hi = rest
    rows = a_ref.shape[2]
    cols = z_ref.shape[1]
    hidden = wo_ref.shape[0]
    lo = min(cols, 128)
    s = pl.program_id(0)

    @pl.when(s < n_mul)
    def _():
        for cc in range(CHAN_BLOCK):
            x = lax.dot_general(a_ref[0, cc], b_ref[0, cc], (((1,), (1,)), ((), ())), preferred_element_type=F32)
            at = pl.multiple_of((s * CHAN_BLOCK + cc) * rows, 8)
            x_lo[pl.ds(at, rows), :lo] = x[:, :lo]
            if cols > lo:
                x_hi[pl.ds(at, rows), :cols - lo] = x[:, lo:]

    @pl.when(s >= n_mul)
    def _():
        first = (s - n_mul) * GROUP
        ln = lnz_ref[...]
        w_g = wg_ref[...]
        w_o = wo_ref[...]
        gain = lnx_ref[:, 0:1]
        bias = lnx_ref[:, 1:2]
        for ii in range(GROUP):
            x = x_lo[pl.ds(first + ii, hidden, stride=rows), :][:, :lo]
            if cols > lo:
                x = jnp.concatenate([x, x_hi[pl.ds(first + ii, hidden, stride=rows), :][:, :cols - lo]], axis=1)
            mean = jnp.mean(x, axis=0, keepdims=True)
            centered = x - mean
            variance = jnp.mean(centered * centered, axis=0, keepdims=True)
            xn = (centered * lax.rsqrt(variance + LN_EPS) * gain + bias).astype(BF16)
            y = lax.dot_general(xn, w_o, (((0,), (0,)), ((), ())), preferred_element_type=F32)
            z = z_ref[ii]
            zn = layer_norm_rows(z, ln).astype(BF16)
            gate = sigmoid(jnp.dot(zn, w_g, preferred_element_type=F32))
            new = z + gate * y
            out_ref[ii] = new
            if emit:
                zn2 = layer_norm_rows(new, ln2_ref[...]) * mask_ref[0][:, ii:ii + 1]
                turn[pl.ds(ii, cols, stride=GROUP), :] = zn2
        if emit:
            next_ref[0] = turn[...].reshape(cols, GROUP, turn.shape[1]).astype(BF16)


def finish(ab, z, ln_z, w_g, ln_x, w_o, slot, extra=None, n_slots=0):
    rows, cols, width = z.shape
    hidden, depth = ab.shape[1], ab.shape[3]
    n_mul = hidden // CHAN_BLOCK
    groups = rows // GROUP

    def tile(i, sl):
        return (jnp.maximum(i - n_mul, 0), 0, 0)

    def whole(i, sl):
        return (0, 0)

    in_specs = [
        pl.BlockSpec((1, CHAN_BLOCK, rows, depth), lambda i, sl: (0, jnp.minimum(i, n_mul - 1), 0, 0)),
        pl.BlockSpec((1, CHAN_BLOCK, rows, depth), lambda i, sl: (1, jnp.minimum(i, n_mul - 1), 0, 0)),
        pl.BlockSpec((GROUP, cols, width), tile),
        pl.BlockSpec((2, width), whole),
        pl.BlockSpec((width, width), whole),
        pl.BlockSpec((hidden, 2), whole),
        pl.BlockSpec((hidden, width), whole),
    ]
    args = [ab, ab, z, ln_z, w_g, ln_x, w_o]
    out_shape = [jax.ShapeDtypeStruct(z.shape, F32)]
    out_specs = [pl.BlockSpec((GROUP, cols, width), tile)]
    scratch = [pltpu.VMEM((hidden * rows, 128), F32), pltpu.VMEM((hidden * rows, 128), F32)]
    if extra is not None:
        in_specs += [pl.BlockSpec((1, cols, GROUP), tile), pl.BlockSpec((2, width), whole)]
        args += list(extra)
        out_shape.append(jax.ShapeDtypeStruct((n_slots, cols, rows, width), BF16))
        out_specs.append(pl.BlockSpec((1, cols, GROUP, width), lambda i, sl: (sl[0], 0, jnp.maximum(i - n_mul, 0), 0)))
        scratch.append(pltpu.VMEM((cols * GROUP, width), F32))
    return pl.pallas_call(
        functools.partial(finish_kernel, n_mul, extra is not None),
        out_shape=out_shape,
        grid_spec=pltpu.PrefetchScalarGridSpec(
            num_scalar_prefetch=1, grid=(n_mul + groups,), in_specs=in_specs, out_specs=out_specs, scratch_shapes=scratch
        ),
        compiler_params=pltpu.CompilerParams(vmem_limit_bytes=62 * 1024 * 1024),
        name="finish",
    )(slot, *args)


def solution(mesh):
    n_z = mesh.shape["dap2"]
    n_r = mesh.shape["dap"]
    pair_spec = P(("data", "dap"), "dap2", None)
    mask_spec = P(("data", "dap"), "dap2")
    out_sems = [(n_z, CHUNKS)] * 7
    in_sems = [(n_z, CHUNKS)] * 5 + [(CHUNKS,)] * 2 + [(n_r, CHUNKS), (CHUNKS,)]

    def local_stack(pair_act, pair_mask, ln_z, w_ab, w_g, ln_x, w_o):
        z_at = lax.axis_index("dap2").astype(jnp.int32)
        r_at = lax.axis_index("dap").astype(jnp.int32)
        slot = z_at.reshape(1)
        rows, cols, _ = pair_act.shape
        mask_g = pair_mask.astype(F32).T.reshape(cols, rows // GROUP, GROUP).transpose(1, 0, 2)
        k = jnp.arange(n_z, dtype=jnp.int32)
        diag = r_at == z_at
        slots_out = jnp.concatenate([k, jnp.where(diag, k, n_z + k)])
        b_in = jnp.where(k == r_at, z_at, 2 * n_z + k)
        a_in = jnp.where(diag, b_in, jnp.where(k == r_at, r_at, n_z + k))
        slots_in = jnp.concatenate([a_in, b_in])

        state = pair_act
        layers = w_o.shape[0]
        buf = None
        for layer in range(layers):
            for upd in range(2):
                lnz = ln_z[layer, upd].astype(F32)
                w_abt = w_ab[layer, upd].T.reshape(2, -1, w_ab.shape[2])
                lnx = ln_x[layer, upd].astype(F32).T
                if buf is None:
                    buf = first_norm(state, mask_g, lnz, slot, 2 * n_z)
                if upd == 0:
                    buf = relay(functools.partial(relay_out_kernel, n_z), buf, out_sems, 2 * layer, f"relay_out_{layer}")
                    ab = project(buf, slots_out, w_abt)
                    nxt = (mask_g, ln_z[layer, 1].astype(F32))
                    state, buf = finish(ab, state, lnz, w_g[layer, 0], lnx, w_o[layer, 0], slot, nxt, 3 * n_z)
                else:
                    buf = relay(functools.partial(relay_in_kernel, n_z), buf, in_sems, 2 * layer + 1, f"relay_in_{layer}")
                    ab = project(buf, slots_in, w_abt)
                    (state,) = finish(ab, state, lnz, w_g[layer, 1], lnx, w_o[layer, 1], slot)
                    buf = None
        return state

    return jax.shard_map(local_stack, mesh=mesh, in_specs=(pair_spec, mask_spec, P(), P(), P(), P(), P()), out_specs=pair_spec, check_vma=False)
```

```python
import functools

import jax
import jax.numpy as jnp
from jax import lax
from jax.experimental import pallas as pl
from jax.experimental.pallas import tpu as pltpu
from jax.sharding import PartitionSpec as P

LN_EPS = 1e-5
GROUP = 16
CHAN_BLOCK = 16
PITCH = 24
PAD = 8
LAG_B = 3
LAG_A = 2
F32 = jnp.float32
BF16 = jnp.bfloat16
MESH = pl.DeviceIdType.MESH


def sigmoid(v):
    return 0.5 * jnp.tanh(0.5 * v) + 0.5


def layer_norm_rows(v, params):
    mean = jnp.mean(v, axis=-1, keepdims=True)
    centered = v - mean
    variance = jnp.mean(centered * centered, axis=-1, keepdims=True)
    return centered * lax.rsqrt(variance + LN_EPS) * params[0:1, :] + params[1:2, :]


def greet(z, r, n_z):
    barrier = pltpu.get_barrier_semaphore()

    def hello(where):
        pl.semaphore_signal(barrier, inc=1, device_id=where, device_id_type=MESH)

    for m in (1, 2, 3):
        hello({"dap": r ^ m})
    pl.when(z > 0)(lambda: hello({"dap2": z - 1}))
    pl.when(z < n_z - 1)(lambda: hello({"dap2": z + 1}))
    inner = (z > 0) & (z < n_z - 1)
    pl.when(inner)(lambda: pl.semaphore_wait(barrier, 5))
    pl.when(jnp.logical_not(inner))(lambda: pl.semaphore_wait(barrier, 4))


def copy_to(buf, src, dst, h, send_sem, recv_sem, where):
    rows = pl.ds(h * GROUP, GROUP)
    return pltpu.make_async_remote_copy(
        src_ref=buf.at[src, rows],
        dst_ref=buf.at[dst, rows],
        send_sem=send_sem,
        recv_sem=recv_sem,
        device_id=where,
        device_id_type=MESH,
    )


def line_copies(buf, z, send_r, send_l, recv_z):
    def right(slot, h):
        return copy_to(buf, slot, slot, h, send_r.at[slot, h], recv_z.at[slot, h], {"dap2": z + 1})

    def left(slot, h):
        return copy_to(buf, slot, slot, h, send_l.at[slot, h], recv_z.at[slot, h], {"dap2": z - 1})

    return right, left


def start_line(right, left, z, h, n_z):
    pl.when(z < n_z - 1)(lambda: right(z, h).start())
    pl.when(z > 0)(lambda: left(z, h).start())


def arrive_line(right, left, z, t, h, n_z, on_arrival):
    @pl.when(z - t >= 0)
    def _():
        right(z - t, h).wait_recv()
        pl.when(z < n_z - 1)(lambda: right(z - t, h).start())
        on_arrival(z - t, h)

    @pl.when(z + t < n_z)
    def _():
        left(z + t, h).wait_recv()
        pl.when(z > 0)(lambda: left(z + t, h).start())
        on_arrival(z + t, h)


def drain_line(right, left, z, n_z, chunks):
    for t in range(n_z):
        @pl.loop(0, chunks)
        def _(h):
            pl.when((z - t >= 0) & (z < n_z - 1))(lambda: right(z - t, h).wait_send())
            pl.when((z + t < n_z) & (z > 0))(lambda: left(z + t, h).wait_send())


class Projector:
    def __init__(self, buf, w_ref, ab, x_in, staged, stage, in_sem, out_sem, sources):
        self.refs = buf, w_ref, ab, x_in, staged, stage
        self.sems = in_sem, out_sem
        self.sources = sources

    def load(self, o, h, k):
        buf, _, _, x_in, _, _ = self.refs
        return pltpu.make_async_copy(buf.at[self.sources[o](k), pl.ds(h * GROUP, GROUP)], x_in.at[o, k], self.sems[0].at[o, k])

    def save(self, o, h):
        _, _, ab, _, staged, _ = self.refs
        return pltpu.make_async_copy(staged.at[o], ab.at[o, :, pl.ds(h * GROUP, GROUP)], self.sems[1].at[o])

    def fetch(self, o, h):
        for k in range(4):
            self.load(o, h, k).start()

    def run(self, o, h):
        _, w_ref, _, x_in, staged, stage = self.refs
        hidden = staged.shape[1]
        parts = staged.shape[3] // 128
        for k in range(4):
            self.load(o, h, k).wait()
        w_t = w_ref[o]

        def one_row(ii, carry):
            zn = jnp.concatenate([x_in[o, k, ii] for k in range(4)], axis=0)
            q = lax.dot_general(w_t, zn, (((1,), (1,)), ((), ())), preferred_element_type=F32)
            val = sigmoid(q[hidden:]) * q[:hidden]
            for p in range(parts):
                stage[p, pl.ds(ii, hidden, stride=PITCH), :] = val[:, p * 128:(p + 1) * 128]
            return carry

        lax.fori_loop(0, GROUP, one_row, 0, unroll=2)
        pl.when(h > 0)(lambda: self.save(o, h - 1).wait())
        for p in range(parts):
            full = stage[p].reshape(hidden, PITCH, 128)
            staged[o, :, :, p * 128:(p + 1) * 128] = full[:, :GROUP].astype(BF16)
        self.save(o, h).start()


class Preparer:
    def __init__(self, turned, z_ref, mask_ref, ln_ref, wg_ref, buf, gate, z_in, z_turned, z_out, g_out, sems, own):
        self.turned = turned
        self.z_turned = z_turned
        self.refs = z_ref, mask_ref, ln_ref, wg_ref, buf, gate
        self.scratch = z_in, z_out, g_out
        self.sems = sems
        self.own = own

    def load(self, h, turned):
        z_ref = self.refs[0]
        rows = pl.ds(h * GROUP, GROUP)
        if turned:
            return pltpu.make_async_copy(z_ref.at[:, rows], self.z_turned.at[h % 2], self.sems.at[0, h % 2])
        return pltpu.make_async_copy(z_ref.at[rows], self.scratch[0].at[h % 2], self.sems.at[0, h % 2])

    def save_own(self, h):
        return pltpu.make_async_copy(self.scratch[1].at[h % 2], self.refs[4].at[self.own, pl.ds(h * GROUP, GROUP)], self.sems.at[1, h % 2])

    def save_gate(self, h):
        return pltpu.make_async_copy(self.scratch[2].at[h % 2], self.refs[5].at[pl.ds(h * GROUP, GROUP)], self.sems.at[2, h % 2])

    def own_chunk(self, h, chunks):
        _, mask_ref, ln_ref, _, _, _ = self.refs
        z_in, z_out, _ = self.scratch
        pl.when(h + 1 < chunks)(lambda: self.load(h + 1, self.turned).start())
        self.load(h, self.turned).wait()
        ln = ln_ref[...]
        mask = mask_ref[h]
        for ii in range(GROUP):
            if self.turned:
                z = self.z_turned[h % 2, :, ii, :]
            else:
                z = z_in[h % 2, ii]
            z_out[h % 2, ii] = (layer_norm_rows(z, ln) * mask[:, ii:ii + 1]).astype(BF16)
        self.save_own(h).start()
        self.save_own(h).wait()

    def gate_chunk(self, h, chunks):
        _, _, ln_ref, wg_ref, _, _ = self.refs
        z_in, _, g_out = self.scratch
        pl.when(h + 1 < chunks)(lambda: self.load(h + 1, False).start())
        self.load(h, False).wait()
        pl.when(h >= 2)(lambda: self.save_gate(h - 2).wait())
        ln = ln_ref[...]
        w_g = wg_ref[...]
        for ii in range(GROUP):
            zn = layer_norm_rows(z_in[h % 2, ii], ln).astype(BF16)
            g_out[h % 2, ii] = sigmoid(jnp.dot(zn, w_g, preferred_element_type=F32))
        self.save_gate(h).start()

    def end_gate(self, chunks):
        for h in range(max(0, chunks - 2), chunks):
            self.save_gate(h).wait()


def relay_out_kernel(n_z, z_ref, mask_ref, ln_ref, wg_ref, w_ref, buf, ab, gate, z_in, z_turned, z_out, g_out, prep_sem,
                     x_in, staged, stage, in_sem, out_sem, send_r, send_l, recv_z, send_p, send_q, recv_b, send_f):
    z = lax.axis_index("dap2")
    r = lax.axis_index("dap")
    chunks = buf.shape[1] // GROUP
    prep = Preparer(False, z_ref, mask_ref, ln_ref, wg_ref, buf, gate, z_in, z_turned, z_out, g_out, prep_sem, z)
    prep.load(0, False).start()
    greet(z, r, n_z)
    right, left = line_copies(buf, z, send_r, send_l, recv_z)
    b_base = jnp.where(r == z, 0, n_z)
    proj = Projector(buf, w_ref, ab, x_in, staged, stage, in_sem, out_sem, (lambda k: k, lambda k: b_base + k))

    def to_near(slot, h):
        return copy_to(buf, slot, n_z + slot, h, send_p.at[slot, h], recv_b.at[slot, h], {"dap": r ^ 1})

    def to_far(slot, h):
        return copy_to(buf, slot, n_z + slot, h, send_q.at[slot, h], recv_b.at[slot, h], {"dap": r ^ 2})

    def onward(slot, h):
        return copy_to(buf, n_z + slot, n_z + slot, h, send_f.at[slot, h], recv_b.at[slot, h], {"dap": r ^ 1})

    def spread(slot, h):
        @pl.when(r == z)
        def _():
            to_far(slot, h).start()
            to_near(slot, h).start()

    def pass_on(slot, h):
        @pl.when(r == z ^ 2)
        def _():
            onward(slot, h).wait_recv()
            onward(slot, h).start()

    def pass_on_step(t, h):
        pl.when(z - t >= 0)(lambda: pass_on(z - t, h))
        pl.when(z + t < n_z)(lambda: pass_on(z + t, h))

    def land_b(h):
        @pl.when((r == z ^ 1) | (r == z ^ 3))
        def _():
            for slot in range(n_z):
                onward(slot, h).wait_recv()

    @pl.loop(0, chunks)
    def _(h):
        prep.own_chunk(h, chunks)
        start_line(right, left, z, h, n_z)
        spread(z, h)

    prep.load(0, False).start()

    @pl.loop(0, chunks)
    def _(h):
        arrive_line(right, left, z, 1, h, n_z, spread)
        prep.gate_chunk(h, chunks)
        pass_on(z, h)
        pl.when(h >= 2)(lambda: pass_on_step(1, h - 2))

    @pl.loop(0, chunks)
    def _(h):
        arrive_line(right, left, z, 2, h, n_z, spread)
        pl.when(h >= 2)(lambda: pass_on_step(2, h - 2))
        pl.when(h < 2)(lambda: pass_on_step(1, h + chunks - 2))

    @pl.loop(0, chunks + LAG_B)
    def _(h):
        @pl.when(h < chunks)
        def _():
            arrive_line(right, left, z, 3, h, n_z, spread)
            proj.fetch(0, h)

        pl.when(h < 2)(lambda: pass_on_step(2, h + chunks - 2))
        pl.when((h >= 2) & (h < chunks + 2))(lambda: pass_on_step(3, h - 2))

        @pl.when(h >= LAG_B)
        def _():
            land_b(h - LAG_B)
            proj.fetch(1, h - LAG_B)

        pl.when(h < chunks)(lambda: proj.run(0, h))
        pl.when(h >= LAG_B)(lambda: proj.run(1, h - LAG_B))

    prep.end_gate(chunks)
    for o in range(2):
        proj.save(o, chunks - 1).wait()
    drain_line(right, left, z, n_z, chunks)
    for slot in range(n_z):
        @pl.loop(0, chunks)
        def _(h):
            @pl.when(r == z)
            def _():
                to_far(slot, h).wait_send()
                to_near(slot, h).wait_send()

            pl.when(r == z ^ 2)(lambda: onward(slot, h).wait_send())


def relay_in_kernel(n_z, z_ref, mask_ref, ln_ref, wg_ref, w_ref, buf, ab, gate, z_in, z_turned, z_out, g_out, prep_sem,
                    x_in, staged, stage, in_sem, out_sem, send_r, send_l, recv_z, send_a, recv_a, recv_b, send_p, send_q, send_f):
    z = lax.axis_index("dap2")
    r = lax.axis_index("dap")
    chunks = buf.shape[1] // GROUP
    prep = Preparer(True, z_ref, mask_ref, ln_ref, wg_ref, buf, gate, z_in, z_turned, z_out, g_out, prep_sem, z)
    prep.load(0, True).start()
    greet(z, r, n_z)
    right, left = line_copies(buf, z, send_r, send_l, recv_z)

    def b_source(k):
        return jnp.where(r == k, z, 2 * n_z + k)

    def a_source(k):
        return jnp.where(r == z, b_source(k), jnp.where(r == k, k, n_z + k))

    proj = Projector(buf, w_ref, ab, x_in, staged, stage, in_sem, out_sem, (a_source, b_source))

    def to_owner(slot, h):
        return copy_to(buf, slot, n_z + r, h, send_a.at[slot, h], recv_a.at[r, h], {"dap": slot})

    def from_peer(peer, h):
        return copy_to(buf, r, n_z + peer, h, send_a.at[peer, h], recv_a.at[peer, h], {"dap": peer})

    def to_near(h):
        return copy_to(buf, z, 2 * n_z + r, h, send_p.at[h], recv_b.at[r, h], {"dap": r ^ 1})

    def to_far(h):
        return copy_to(buf, z, 2 * n_z + r, h, send_q.at[h], recv_b.at[r, h], {"dap": r ^ 2})

    def onward(h):
        return copy_to(buf, 2 * n_z + (r ^ 2), 2 * n_z + (r ^ 2), h, send_f.at[h], recv_b.at[r ^ 2, h], {"dap": r ^ 1})

    def from_b(peer, h):
        return copy_to(buf, z, 2 * n_z + peer, h, send_p.at[h], recv_b.at[peer, h], {"dap": r ^ 1})

    def spread(slot, h):
        pl.when(slot != r)(lambda: to_owner(slot, h).start())

    @pl.loop(0, chunks)
    def _(h):
        prep.own_chunk(h, chunks)
        start_line(right, left, z, h, n_z)
        to_far(h).start()
        to_near(h).start()

    prep.load(0, False).start()

    @pl.loop(0, chunks)
    def _(h):
        arrive_line(right, left, z, 1, h, n_z, spread)
        prep.gate_chunk(h, chunks)

    @pl.loop(0, chunks)
    def _(h):
        arrive_line(right, left, z, 2, h, n_z, spread)
        onward(h).wait_recv()
        onward(h).start()

    @pl.loop(0, chunks + LAG_A)
    def _(h):
        @pl.when(h < chunks)
        def _():
            arrive_line(right, left, z, 3, h, n_z, spread)
            from_b(r ^ 1, h).wait_recv()
            from_b(r ^ 3, h).wait_recv()
            proj.fetch(1, h)

        @pl.when(h >= LAG_A)
        def _():
            @pl.when(r != z)
            def _():
                for m in (1, 2, 3):
                    from_peer(r ^ m, h - LAG_A).wait_recv()

            proj.fetch(0, h - LAG_A)

        pl.when(h < chunks)(lambda: proj.run(1, h))
        pl.when(h >= LAG_A)(lambda: proj.run(0, h - LAG_A))

    prep.end_gate(chunks)
    for o in range(2):
        proj.save(o, chunks - 1).wait()
    drain_line(right, left, z, n_z, chunks)

    @pl.loop(0, chunks)
    def _(h):
        to_far(h).wait_send()
        to_near(h).wait_send()
        onward(h).wait_send()
        for slot in range(n_z):
            pl.when((slot != z) & (slot != r))(lambda: to_owner(slot, h).wait_send())


def relay(kernel, n_slots, state, mask_g, ln, w_g, w_abt, sems, collective_id, name):
    rows, cols, width = state.shape
    hidden = w_abt.shape[1] // 2
    depth = 4 * cols
    in_hbm = pl.BlockSpec(memory_space=pl.ANY)
    in_vmem = pl.BlockSpec(memory_space=pltpu.VMEM)
    return pl.pallas_call(
        kernel,
        out_shape=[
            jax.ShapeDtypeStruct((n_slots, rows, cols, width), BF16),
            jax.ShapeDtypeStruct((2, hidden, rows, depth), BF16),
            jax.ShapeDtypeStruct(state.shape, F32),
        ],
        in_specs=[in_hbm, in_vmem, in_vmem, in_vmem, in_vmem],
        out_specs=[in_hbm, in_hbm, in_hbm],
        scratch_shapes=[
            pltpu.VMEM((2, GROUP, cols, width), F32),
            pltpu.VMEM((2, rows, GROUP, width), F32),
            pltpu.VMEM((2, GROUP, cols, width), BF16),
            pltpu.VMEM((2, GROUP, cols, width), F32),
            pltpu.SemaphoreType.DMA((3, 2)),
            pltpu.VMEM((2, 4, GROUP, cols, width), BF16),
            pltpu.VMEM((2, hidden, GROUP, depth), BF16),
            pltpu.VMEM((depth // 128, hidden * PITCH, 128), F32),
            pltpu.SemaphoreType.DMA((2, 4)),
            pltpu.SemaphoreType.DMA((2,)),
        ] + [pltpu.SemaphoreType.DMA(s) for s in sems],
        compiler_params=pltpu.CompilerParams(
            collective_id=collective_id, has_side_effects=True, vmem_limit_bytes=48 * 1024 * 1024
        ),
        name=name,
    )(state, mask_g, ln, w_g, w_abt)[1:]


def finish_kernel(n_mul, a_ref, b_ref, z_ref, gate_ref, lnx_ref, wo_ref, out_ref, x_lo, x_hi):
    rows = a_ref.shape[2]
    cols = z_ref.shape[1]
    hidden = wo_ref.shape[0]
    lo = min(cols, 128)
    s = pl.program_id(0)

    @pl.when(s < n_mul)
    def _():
        for cc in range(CHAN_BLOCK):
            x = lax.dot_general(a_ref[0, cc], b_ref[0, cc], (((1,), (1,)), ((), ())), preferred_element_type=F32)
            at = pl.multiple_of((s * CHAN_BLOCK + cc) * (rows + PAD), 8)
            x_lo[pl.ds(at, rows), :lo] = x[:, :lo]
            if cols > lo:
                x_hi[pl.ds(at, rows), :cols - lo] = x[:, lo:]

    @pl.when(s >= n_mul)
    def _():
        first = (s - n_mul) * GROUP
        w_o = wo_ref[...]
        gain = lnx_ref[:, 0:1]
        bias = lnx_ref[:, 1:2]

        def normed(x):
            mean = jnp.mean(x, axis=0, keepdims=True)
            centered = x - mean
            variance = jnp.mean(centered * centered, axis=0, keepdims=True)
            return (centered * lax.rsqrt(variance + LN_EPS) * gain + bias).astype(BF16)

        for ii in range(GROUP):
            row = pl.ds(first + ii, hidden, stride=rows + PAD)
            xn = normed(x_lo[row, :][:, :lo])
            if cols > lo:
                xn = jnp.concatenate([xn, normed(x_hi[row, :][:, :cols - lo])], axis=1)
            y = lax.dot_general(xn, w_o, (((0,), (0,)), ((), ())), preferred_element_type=F32)
            out_ref[ii] = z_ref[ii] + gate_ref[ii] * y


def finish(ab, z, gate, ln_x, w_o):
    rows, cols, width = z.shape
    hidden, depth = ab.shape[1], ab.shape[3]
    n_mul = hidden // CHAN_BLOCK

    def tile(i):
        return (jnp.maximum(i - n_mul, 0), 0, 0)

    def whole(i):
        return (0, 0)

    return pl.pallas_call(
        functools.partial(finish_kernel, n_mul),
        out_shape=jax.ShapeDtypeStruct(z.shape, F32),
        grid=(n_mul + rows // GROUP,),
        in_specs=[
            pl.BlockSpec((1, CHAN_BLOCK, rows, depth), lambda i: (0, jnp.minimum(i, n_mul - 1), 0, 0)),
            pl.BlockSpec((1, CHAN_BLOCK, rows, depth), lambda i: (1, jnp.minimum(i, n_mul - 1), 0, 0)),
            pl.BlockSpec((GROUP, cols, width), tile),
            pl.BlockSpec((GROUP, cols, width), tile),
            pl.BlockSpec((hidden, 2), whole),
            pl.BlockSpec((hidden, width), whole),
        ],
        out_specs=pl.BlockSpec((GROUP, cols, width), tile),
        scratch_shapes=[pltpu.VMEM((hidden * (rows + PAD), 128), F32)] * 2,
        compiler_params=pltpu.CompilerParams(vmem_limit_bytes=62 * 1024 * 1024),
        name="finish",
    )(ab, ab, z, gate, ln_x, w_o)


def solution(mesh):
    n_z = mesh.shape["dap2"]
    pair_spec = P(("data", "dap"), "dap2", None)
    mask_spec = P(("data", "dap"), "dap2")

    def local_stack(pair_act, pair_mask, ln_z, w_ab, w_g, ln_x, w_o):
        rows, cols, _ = pair_act.shape
        chunks = rows // GROUP
        sems = [[(n_z, chunks)] * 7, [(n_z, chunks)] * 6 + [(chunks,)] * 3]
        mask = pair_mask.astype(F32)
        masks = [m.reshape(cols, chunks, GROUP).transpose(1, 0, 2) for m in (mask.T, mask)]
        kernels = [relay_out_kernel, relay_in_kernel]
        state = pair_act
        for layer in range(w_o.shape[0]):
            for upd in range(2):
                ab, gate = relay(
                    functools.partial(kernels[upd], n_z),
                    (2 + upd) * n_z,
                    state,
                    masks[upd],
                    ln_z[layer, upd].astype(F32),
                    w_g[layer, upd],
                    w_ab[layer, upd].T.reshape(2, -1, w_ab.shape[2]),
                    sems[upd],
                    2 * layer + upd,
                    f"relay_{layer}_{upd}",
                )
                state = finish(ab, state, gate, ln_x[layer, upd].astype(F32).T, w_o[layer, upd])
        return state

    return jax.shard_map(local_stack, mesh=mesh, in_specs=(pair_spec, mask_spec, P(), P(), P(), P(), P()), out_specs=pair_spec, check_vma=False)
```

```python
import functools

import jax
import jax.numpy as jnp
from jax import lax
from jax.experimental import pallas as pl
from jax.experimental.pallas import tpu as pltpu
from jax.sharding import PartitionSpec as P

LN_EPS = 1e-5
GROUP = 16
CHAN_BLOCK = 16
PITCH = 24
PAD = 4
LAG_B = 1
LAG_A = 2
F32 = jnp.float32
BF16 = jnp.bfloat16
MESH = pl.DeviceIdType.MESH


def sigmoid(v):
    return 0.5 * jnp.tanh(0.5 * v) + 0.5


def layer_norm_rows(v, params):
    mean = jnp.mean(v, axis=-1, keepdims=True)
    centered = v - mean
    variance = jnp.mean(centered * centered, axis=-1, keepdims=True)
    return centered * lax.rsqrt(variance + LN_EPS) * params[0:1, :] + params[1:2, :]


def greet(z, r, n_z):
    barrier = pltpu.get_barrier_semaphore()

    def hello(where):
        pl.semaphore_signal(barrier, inc=1, device_id=where, device_id_type=MESH)

    for m in (1, 2, 3):
        hello({"dap": r ^ m})
    pl.when(z > 0)(lambda: hello({"dap2": z - 1}))
    pl.when(z < n_z - 1)(lambda: hello({"dap2": z + 1}))


def meet(z, n_z):
    barrier = pltpu.get_barrier_semaphore()
    inner = (z > 0) & (z < n_z - 1)
    pl.when(inner)(lambda: pl.semaphore_wait(barrier, 5))
    pl.when(jnp.logical_not(inner))(lambda: pl.semaphore_wait(barrier, 4))


def copy_to(buf, src, dst, h, send_sem, recv_sem, where):
    rows = pl.ds(h * GROUP, GROUP)
    return pltpu.make_async_remote_copy(
        src_ref=buf.at[src, rows],
        dst_ref=buf.at[dst, rows],
        send_sem=send_sem,
        recv_sem=recv_sem,
        device_id=where,
        device_id_type=MESH,
    )


def line_copies(buf, z, send_r, send_l, recv_z):
    def right(slot, h):
        return copy_to(buf, slot, slot, h, send_r.at[slot, h], recv_z.at[slot, h], {"dap2": z + 1})

    def left(slot, h):
        return copy_to(buf, slot, slot, h, send_l.at[slot, h], recv_z.at[slot, h], {"dap2": z - 1})

    return right, left


def start_line(right, left, z, h, n_z):
    pl.when(z < n_z - 1)(lambda: right(z, h).start())
    pl.when(z > 0)(lambda: left(z, h).start())


def arrive_line(right, left, z, t, h, n_z, on_arrival):
    @pl.when(z - t >= 0)
    def _():
        right(z - t, h).wait_recv()
        pl.when(z < n_z - 1)(lambda: right(z - t, h).start())
        on_arrival(z - t, h)

    @pl.when(z + t < n_z)
    def _():
        left(z + t, h).wait_recv()
        pl.when(z > 0)(lambda: left(z + t, h).start())
        on_arrival(z + t, h)


def drain_line(right, left, z, n_z, chunks):
    for t in range(n_z):
        @pl.loop(0, chunks)
        def _(h):
            pl.when((z - t >= 0) & (z < n_z - 1))(lambda: right(z - t, h).wait_send())
            pl.when((z + t < n_z) & (z > 0))(lambda: left(z + t, h).wait_send())


class Projector:
    def __init__(self, buf, w_ref, ab, x_in, staged, stage, in_sem, out_sem, sources):
        self.refs = buf, w_ref, ab, x_in, staged, stage
        self.sems = in_sem, out_sem
        self.sources = sources

    def load(self, o, h, k):
        buf, _, _, x_in, _, _ = self.refs
        return pltpu.make_async_copy(buf.at[self.sources[o](k), pl.ds(h * GROUP, GROUP)], x_in.at[o, k], self.sems[0].at[o, k])

    def save(self, o, h):
        _, _, ab, _, staged, _ = self.refs
        return pltpu.make_async_copy(staged.at[o], ab.at[o, :, pl.ds(h * GROUP, GROUP)], self.sems[1].at[o])

    def fetch(self, o, h):
        for k in range(4):
            self.load(o, h, k).start()

    def run(self, o, h):
        _, w_ref, _, x_in, staged, stage = self.refs
        hidden = staged.shape[1]
        parts = staged.shape[3] // 128
        for k in range(4):
            self.load(o, h, k).wait()
        w_t = w_ref[o]

        def one_row(ii, carry):
            zn = jnp.concatenate([x_in[o, k, ii] for k in range(4)], axis=0)
            q = lax.dot_general(w_t, zn, (((1,), (1,)), ((), ())), preferred_element_type=F32)
            val = sigmoid(q[hidden:]) * q[:hidden]
            for p in range(parts):
                stage[p, pl.ds(ii, hidden, stride=PITCH), :] = val[:, p * 128:(p + 1) * 128]
            return carry

        lax.fori_loop(0, GROUP, one_row, 0, unroll=8)
        pl.when(h > 0)(lambda: self.save(o, h - 1).wait())
        for p in range(parts):
            full = stage[p].reshape(hidden, PITCH, 128)
            staged[o, :, :, p * 128:(p + 1) * 128] = full[:, :GROUP].astype(BF16)
        self.save(o, h).start()


class Preparer:
    def __init__(self, turned, z_ref, mask_ref, ln_ref, wg_ref, buf, gate, z_in, z_turned, z_out, g_out, sems, own):
        self.turned = turned
        self.z_turned = z_turned
        self.refs = z_ref, mask_ref, ln_ref, wg_ref, buf, gate
        self.scratch = z_in, z_out, g_out
        self.sems = sems
        self.own = own

    def load(self, h, turned):
        z_ref = self.refs[0]
        rows = pl.ds(h * GROUP, GROUP)
        if turned:
            return pltpu.make_async_copy(z_ref.at[:, rows], self.z_turned.at[h % 2], self.sems.at[0, h % 2])
        return pltpu.make_async_copy(z_ref.at[rows], self.scratch[0].at[h % 2], self.sems.at[0, h % 2])

    def save_own(self, h):
        return pltpu.make_async_copy(self.scratch[1].at[h % 2], self.refs[4].at[self.own, pl.ds(h * GROUP, GROUP)], self.sems.at[1, h % 2])

    def save_gate(self, h):
        return pltpu.make_async_copy(self.scratch[2].at[h % 2], self.refs[5].at[pl.ds(h * GROUP, GROUP)], self.sems.at[2, h % 2])

    def own_chunk(self, h, chunks):
        _, mask_ref, ln_ref, _, _, _ = self.refs
        z_in, z_out, _ = self.scratch
        pl.when(h + 1 < chunks)(lambda: self.load(h + 1, self.turned).start())
        self.load(h, self.turned).wait()
        ln = ln_ref[...]
        mask = mask_ref[h]
        for ii in range(GROUP):
            if self.turned:
                z = self.z_turned[h % 2, :, ii, :]
            else:
                z = z_in[h % 2, ii]
            z_out[h % 2, ii] = (layer_norm_rows(z, ln) * mask[:, ii:ii + 1]).astype(BF16)
        self.save_own(h).start()
        self.save_own(h).wait()

    def gate_chunk(self, h, chunks):
        _, _, ln_ref, wg_ref, _, _ = self.refs
        z_in, _, g_out = self.scratch
        pl.when(h + 1 < chunks)(lambda: self.load(h + 1, False).start())
        self.load(h, False).wait()
        pl.when(h >= 2)(lambda: self.save_gate(h - 2).wait())
        ln = ln_ref[...]
        w_g = wg_ref[...]
        for ii in range(GROUP):
            zn = layer_norm_rows(z_in[h % 2, ii], ln).astype(BF16)
            g_out[h % 2, ii] = sigmoid(jnp.dot(zn, w_g, preferred_element_type=F32))
        self.save_gate(h).start()

    def end_gate(self, chunks):
        for h in range(max(0, chunks - 2), chunks):
            self.save_gate(h).wait()


def relay_out_kernel(n_z, z_ref, mask_ref, ln_ref, wg_ref, w_ref, buf, ab, gate, z_in, z_turned, z_out, g_out, prep_sem,
                     x_in, staged, stage, in_sem, out_sem, send_r, send_l, recv_z, send_p, send_q, recv_b, send_f):
    z = lax.axis_index("dap2")
    r = lax.axis_index("dap")
    chunks = buf.shape[1] // GROUP
    prep = Preparer(False, z_ref, mask_ref, ln_ref, wg_ref, buf, gate, z_in, z_turned, z_out, g_out, prep_sem, z)
    prep.load(0, False).start()
    greet(z, r, n_z)
    right, left = line_copies(buf, z, send_r, send_l, recv_z)
    b_base = jnp.where(r == z, 0, n_z)
    proj = Projector(buf, w_ref, ab, x_in, staged, stage, in_sem, out_sem, (lambda k: k, lambda k: b_base + k))

    def to_near(slot, h):
        return copy_to(buf, slot, n_z + slot, h, send_p.at[slot, h], recv_b.at[slot, h], {"dap": r ^ 1})

    def to_far(slot, h):
        return copy_to(buf, slot, n_z + slot, h, send_q.at[slot, h], recv_b.at[slot, h], {"dap": r ^ 2})

    def onward(slot, h):
        return copy_to(buf, n_z + slot, n_z + slot, h, send_f.at[slot, h], recv_b.at[slot, h], {"dap": r ^ 1})

    def spread(slot, h):
        @pl.when(r == z)
        def _():
            to_far(slot, h).start()
            to_near(slot, h).start()

    def pass_on(slot, h):
        @pl.when(r == z ^ 2)
        def _():
            onward(slot, h).wait_recv()
            onward(slot, h).start()

    def pass_on_step(t, h):
        pl.when(z - t >= 0)(lambda: pass_on(z - t, h))
        pl.when(z + t < n_z)(lambda: pass_on(z + t, h))

    def land_b(h):
        @pl.when((r == z ^ 1) | (r == z ^ 3))
        def _():
            for slot in range(n_z):
                onward(slot, h).wait_recv()

    @pl.loop(0, chunks)
    def _(h):
        prep.own_chunk(h, chunks)
        pl.when(h == 0)(lambda: meet(z, n_z))
        start_line(right, left, z, h, n_z)
        spread(z, h)

    prep.load(0, False).start()

    @pl.loop(0, chunks)
    def _(h):
        arrive_line(right, left, z, 1, h, n_z, spread)
        prep.gate_chunk(h, chunks)
        pass_on(z, h)
        pl.when(h >= 1)(lambda: pass_on_step(1, h - 1))

    @pl.loop(0, chunks)
    def _(h):
        arrive_line(right, left, z, 2, h, n_z, spread)
        pl.when(h >= 1)(lambda: pass_on_step(2, h - 1))
        pl.when(h < 1)(lambda: pass_on_step(1, chunks - 1))

    @pl.loop(0, chunks + LAG_B)
    def _(h):
        @pl.when(h < chunks)
        def _():
            arrive_line(right, left, z, 3, h, n_z, spread)
            proj.fetch(0, h)

        pl.when(h < 1)(lambda: pass_on_step(2, chunks - 1))
        pl.when(h >= 1)(lambda: pass_on_step(3, h - 1))

        @pl.when(h >= LAG_B)
        def _():
            land_b(h - LAG_B)
            proj.fetch(1, h - LAG_B)

        pl.when(h < chunks)(lambda: proj.run(0, h))
        pl.when(h >= LAG_B)(lambda: proj.run(1, h - LAG_B))

    prep.end_gate(chunks)
    for o in range(2):
        proj.save(o, chunks - 1).wait()
    drain_line(right, left, z, n_z, chunks)
    for slot in range(n_z):
        @pl.loop(0, chunks)
        def _(h):
            @pl.when(r == z)
            def _():
                to_far(slot, h).wait_send()
                to_near(slot, h).wait_send()

            pl.when(r == z ^ 2)(lambda: onward(slot, h).wait_send())


def relay_in_kernel(n_z, z_ref, mask_ref, ln_ref, wg_ref, w_ref, buf, ab, gate, z_in, z_turned, z_out, g_out, prep_sem,
                    x_in, staged, stage, in_sem, out_sem, send_r, send_l, recv_z, send_a, recv_a, recv_b, send_p, send_q, send_f):
    z = lax.axis_index("dap2")
    r = lax.axis_index("dap")
    chunks = buf.shape[1] // GROUP
    prep = Preparer(True, z_ref, mask_ref, ln_ref, wg_ref, buf, gate, z_in, z_turned, z_out, g_out, prep_sem, z)
    prep.load(0, True).start()
    greet(z, r, n_z)
    right, left = line_copies(buf, z, send_r, send_l, recv_z)

    def b_source(k):
        return jnp.where(r == k, z, 2 * n_z + k)

    def a_source(k):
        return jnp.where(r == z, b_source(k), jnp.where(r == k, k, n_z + k))

    proj = Projector(buf, w_ref, ab, x_in, staged, stage, in_sem, out_sem, (a_source, b_source))

    def to_owner(slot, h):
        return copy_to(buf, slot, n_z + r, h, send_a.at[slot, h], recv_a.at[r, h], {"dap": slot})

    def from_peer(peer, h):
        return copy_to(buf, r, n_z + peer, h, send_a.at[peer, h], recv_a.at[peer, h], {"dap": peer})

    def to_near(h):
        return copy_to(buf, z, 2 * n_z + r, h, send_p.at[h], recv_b.at[r, h], {"dap": r ^ 1})

    def to_far(h):
        return copy_to(buf, z, 2 * n_z + r, h, send_q.at[h], recv_b.at[r, h], {"dap": r ^ 2})

    def onward(h):
        return copy_to(buf, 2 * n_z + (r ^ 2), 2 * n_z + (r ^ 2), h, send_f.at[h], recv_b.at[r ^ 2, h], {"dap": r ^ 1})

    def from_b(peer, h):
        return copy_to(buf, z, 2 * n_z + peer, h, send_p.at[h], recv_b.at[peer, h], {"dap": r ^ 1})

    def spread(slot, h):
        pl.when(slot != r)(lambda: to_owner(slot, h).start())

    @pl.loop(0, chunks)
    def _(h):
        prep.own_chunk(h, chunks)
        pl.when(h == 0)(lambda: meet(z, n_z))
        start_line(right, left, z, h, n_z)
        to_far(h).start()
        to_near(h).start()

    prep.load(0, False).start()

    @pl.loop(0, chunks)
    def _(h):
        arrive_line(right, left, z, 1, h, n_z, spread)
        prep.gate_chunk(h, chunks)

    @pl.loop(0, chunks)
    def _(h):
        arrive_line(right, left, z, 2, h, n_z, spread)
        onward(h).wait_recv()
        onward(h).start()

    @pl.loop(0, chunks + LAG_A)
    def _(h):
        @pl.when(h < chunks)
        def _():
            arrive_line(right, left, z, 3, h, n_z, spread)
            from_b(r ^ 1, h).wait_recv()
            from_b(r ^ 3, h).wait_recv()
            proj.fetch(1, h)

        @pl.when(h >= LAG_A)
        def _():
            @pl.when(r != z)
            def _():
                for m in (1, 2, 3):
                    from_peer(r ^ m, h - LAG_A).wait_recv()

            proj.fetch(0, h - LAG_A)

        pl.when(h < chunks)(lambda: proj.run(1, h))
        pl.when(h >= LAG_A)(lambda: proj.run(0, h - LAG_A))

    prep.end_gate(chunks)
    for o in range(2):
        proj.save(o, chunks - 1).wait()
    drain_line(right, left, z, n_z, chunks)

    @pl.loop(0, chunks)
    def _(h):
        to_far(h).wait_send()
        to_near(h).wait_send()
        onward(h).wait_send()
        for slot in range(n_z):
            pl.when((slot != z) & (slot != r))(lambda: to_owner(slot, h).wait_send())


def relay(kernel, n_slots, state, mask_g, ln, w_g, w_abt, sems, collective_id, name):
    rows, cols, width = state.shape
    hidden = w_abt.shape[1] // 2
    depth = 4 * cols
    in_hbm = pl.BlockSpec(memory_space=pl.ANY)
    in_vmem = pl.BlockSpec(memory_space=pltpu.VMEM)
    return pl.pallas_call(
        kernel,
        out_shape=[
            jax.ShapeDtypeStruct((n_slots, rows, cols, width), BF16),
            jax.ShapeDtypeStruct((2, hidden, rows, depth), BF16),
            jax.ShapeDtypeStruct(state.shape, F32),
        ],
        in_specs=[in_hbm, in_vmem, in_vmem, in_vmem, in_vmem],
        out_specs=[in_hbm, in_hbm, in_hbm],
        scratch_shapes=[
            pltpu.VMEM((2, GROUP, cols, width), F32),
            pltpu.VMEM((2, rows, GROUP, width), F32),
            pltpu.VMEM((2, GROUP, cols, width), BF16),
            pltpu.VMEM((2, GROUP, cols, width), F32),
            pltpu.SemaphoreType.DMA((3, 2)),
            pltpu.VMEM((2, 4, GROUP, cols, width), BF16),
            pltpu.VMEM((2, hidden, GROUP, depth), BF16),
            pltpu.VMEM((depth // 128, hidden * PITCH, 128), F32),
            pltpu.SemaphoreType.DMA((2, 4)),
            pltpu.SemaphoreType.DMA((2,)),
        ] + [pltpu.SemaphoreType.DMA(s) for s in sems],
        compiler_params=pltpu.CompilerParams(
            collective_id=collective_id, has_side_effects=True, vmem_limit_bytes=48 * 1024 * 1024
        ),
        name=name,
    )(state, mask_g, ln, w_g, w_abt)[1:]


def finish_kernel(n_mul, a_ref, b_ref, z_ref, gate_ref, lnx_ref, wo_ref, out_ref, x_lo, x_hi):
    rows = a_ref.shape[2]
    cols = z_ref.shape[1]
    hidden = wo_ref.shape[0]
    lo = min(cols, 128)
    s = pl.program_id(0)

    @pl.when(s < n_mul)
    def _():
        for cc in range(CHAN_BLOCK):
            x = lax.dot_general(a_ref[0, cc], b_ref[0, cc], (((1,), (1,)), ((), ())), preferred_element_type=F32)
            at = pl.multiple_of(s * (CHAN_BLOCK * (rows + PAD)), 8) + cc * (rows + PAD)
            x_lo[pl.ds(at, rows), :lo] = x[:, :lo]
            if cols > lo:
                x_hi[pl.ds(at, rows), :cols - lo] = x[:, lo:]

    @pl.when(s >= n_mul)
    def _():
        first = (s - n_mul) * GROUP
        w_o = wo_ref[...]
        gain = lnx_ref[:, 0:1]
        bias = lnx_ref[:, 1:2]

        def normed(x):
            mean = jnp.mean(x, axis=0, keepdims=True)
            centered = x - mean
            variance = jnp.mean(centered * centered, axis=0, keepdims=True)
            return (centered * lax.rsqrt(variance + LN_EPS) * gain + bias).astype(BF16)

        for ii in range(GROUP):
            row = pl.ds(first + ii, hidden, stride=rows + PAD)
            xn = normed(x_lo[row, :][:, :lo])
            if cols > lo:
                xn = jnp.concatenate([xn, normed(x_hi[row, :][:, :cols - lo])], axis=1)
            y = lax.dot_general(xn, w_o, (((0,), (0,)), ((), ())), preferred_element_type=F32)
            out_ref[ii] = z_ref[ii] + gate_ref[ii] * y


def finish(ab, z, gate, ln_x, w_o):
    rows, cols, width = z.shape
    hidden, depth = ab.shape[1], ab.shape[3]
    n_mul = hidden // CHAN_BLOCK

    def tile(i):
        return (jnp.maximum(i - n_mul, 0), 0, 0)

    def whole(i):
        return (0, 0)

    return pl.pallas_call(
        functools.partial(finish_kernel, n_mul),
        out_shape=jax.ShapeDtypeStruct(z.shape, F32),
        grid=(n_mul + rows // GROUP,),
        in_specs=[
            pl.BlockSpec((1, CHAN_BLOCK, rows, depth), lambda i: (0, jnp.minimum(i, n_mul - 1), 0, 0)),
            pl.BlockSpec((1, CHAN_BLOCK, rows, depth), lambda i: (1, jnp.minimum(i, n_mul - 1), 0, 0)),
            pl.BlockSpec((GROUP, cols, width), tile),
            pl.BlockSpec((GROUP, cols, width), tile),
            pl.BlockSpec((hidden, 2), whole),
            pl.BlockSpec((hidden, width), whole),
        ],
        out_specs=pl.BlockSpec((GROUP, cols, width), tile),
        scratch_shapes=[pltpu.VMEM((hidden * (rows + PAD), 128), F32)] * 2,
        compiler_params=pltpu.CompilerParams(vmem_limit_bytes=62 * 1024 * 1024),
        name="finish",
    )(ab, ab, z, gate, ln_x, w_o)


def solution(mesh):
    n_z = mesh.shape["dap2"]
    pair_spec = P(("data", "dap"), "dap2", None)
    mask_spec = P(("data", "dap"), "dap2")

    def local_stack(pair_act, pair_mask, ln_z, w_ab, w_g, ln_x, w_o):
        rows, cols, _ = pair_act.shape
        chunks = rows // GROUP
        sems = [[(n_z, chunks)] * 7, [(n_z, chunks)] * 6 + [(chunks,)] * 3]
        mask = pair_mask.astype(F32)
        masks = [m.reshape(cols, chunks, GROUP).transpose(1, 0, 2) for m in (mask.T, mask)]
        kernels = [relay_out_kernel, relay_in_kernel]
        state = pair_act
        for layer in range(w_o.shape[0]):
            for upd in range(2):
                ab, gate = relay(
                    functools.partial(kernels[upd], n_z),
                    (2 + upd) * n_z,
                    state,
                    masks[upd],
                    ln_z[layer, upd].astype(F32),
                    w_g[layer, upd],
                    w_ab[layer, upd].T.reshape(2, -1, w_ab.shape[2]),
                    sems[upd],
                    2 * layer + upd,
                    f"relay_{layer}_{upd}",
                )
                state = finish(ab, state, gate, ln_x[layer, upd].astype(F32).T, w_o[layer, upd])
        return state

    return jax.shard_map(local_stack, mesh=mesh, in_specs=(pair_spec, mask_spec, P(), P(), P(), P(), P()), out_specs=pair_spec, check_vma=False)
```
